32 devices in a mesh: replica: 16 (over z, y, x), model: 2 (over core).
Axes of the slice: x: 2, y: 2, z: 4, core: 2. Of those that a mesh axis runs over, the one named last changes fastest.
Arguments:
- slope_up: float32 [16, 768, 3072], P('replica', None, 'model'), may hold values from -4 to 4
- slope_down: float32 [16, 3072, 768], P('replica', 'model'), may hold values from -4 to 4
- slope_query: float32 [16, 768, 768], P('replica', None, 'model'), may hold values from -4 to 4
- slope_key: float32 [16, 768, 768], P('replica', None, 'model'), may hold values from -4 to 4
- slope_value: float32 [16, 768, 768], P('replica', None, 'model'), may hold values from -4 to 4
- slope_mixed: float32 [16, 768, 768], P('replica', 'model'), may hold values from -4 to 4
- slope_norm: float32 [16, 768], P('replica'), may hold values from -8 to 8
- slope_bias: float32 [16, 768], P('replica'), may hold values from -8 to 8
- param_up: float32 [768, 3072], P('replica', 'model'), may hold values from -0.3125 to 0.3125
- param_down: float32 [3072, 768], P('model', 'replica'), may hold values from -0.15625 to 0.15625
- param_query: float32 [768, 768], P('replica', 'model'), may hold values from -0.3125 to 0.3125
- param_key: float32 [768, 768], P('replica', 'model'), may hold values from -0.3125 to 0.3125
- param_value: float32 [768, 768], P('replica', 'model'), may hold values from -0.3125 to 0.3125
- param_mixed: float32 [768, 768], P('model', 'replica'), may hold values from -0.3125 to 0.3125
- param_norm: float32 [768], P('replica'), may hold values from 0.25 to 1.75
- param_bias: float32 [768], P('replica'), may hold values from -3 to 3
- state_up: float32 [768, 3072], P('replica', 'model'), may hold values from 0.00026041668 to 0.0026041667
- state_down: float32 [3072, 768], P('model', 'replica'), may hold values from 6.510417e-05 to 0.0006510417
- state_query: float32 [768, 768], P('replica', 'model'), may hold values from 0.00026041668 to 0.0026041667
- state_key: float32 [768, 768], P('replica', 'model'), may hold values from 0.00026041668 to 0.0026041667
- state_value: float32 [768, 768], P('replica', 'model'), may hold values from 0.00026041668 to 0.0026041667
- state_mixed: float32 [768, 768], P('model', 'replica'), may hold values from 0.00026041668 to 0.0026041667
- state_norm: float32 [768], P('replica'), may hold values from 0.05 to 0.8
- state_bias: float32 [768], P('replica'), may hold values from 0.05 to 0.8
Outputs:
- half_up: bfloat16 [768, 3072], P(None, 'model')
- half_down: bfloat16 [3072, 768], P('model')
- half_query: bfloat16 [768, 768], P(None, 'model')
- half_key: bfloat16 [768, 768], P(None, 'model')
- half_value: bfloat16 [768, 768], P(None, 'model')
- half_mixed: bfloat16 [768, 768], P('model')
- half_norm: bfloat16 [768], replicated
- half_bias: bfloat16 [768], replicated
- next_up: float32 [768, 3072], P('replica', 'model')
- next_down: float32 [3072, 768], P('model', 'replica')
- next_query: float32 [768, 768], P('replica', 'model')
- next_key: float32 [768, 768], P('replica', 'model')
- next_value: float32 [768, 768], P('replica', 'model')
- next_mixed: float32 [768, 768], P('model', 'replica')
- next_norm: float32 [768], P('replica')
- next_bias: float32 [768], P('replica')
- state_new_up: float32 [768, 3072], P('replica', 'model')
- state_new_down: float32 [3072, 768], P('model', 'replica')
- state_new_query: float32 [768, 768], P('replica', 'model')
- state_new_key: float32 [768, 768], P('replica', 'model')
- state_new_value: float32 [768, 768], P('replica', 'model')
- state_new_mixed: float32 [768, 768], P('model', 'replica')
- state_new_norm: float32 [768], P('replica')
- state_new_bias: float32 [768], P('replica')
The draws below stay inside these ranges and needn't reach their ends.
All inputs are finite; a program needn't handle non-finite values.
Results may differ from the reference program's by a relative error of at most 0.001.
Values may be sent and summed in bfloat16 or wider, within the bound.
A program may use at most 64 MiB of HBM per device.

```python
import jax
import jax.numpy as jnp
from jax import lax

WIDTH = 768
INNER = 3072
ATTN = 768
REPLICAS = 16


def with_spikes(array, rng, source, target, parts, factor):
    owner, partner = [(jnp.arange(array.shape[axis_at]) // (array.shape[axis_at] // parts)).reshape([-1 if axis == axis_at else 1 for axis in range(array.ndim)]) for axis_at in (source, target)]
    chosen = jax.random.permutation(rng, parts)[partner]
    strong = (owner == chosen) | (owner == (partner + parts // 2) % parts)
    return jnp.where(strong, factor * array, array)


def shard_levels(rng, extent, split, low, top_value):
    factor_of, own = 1.0, jax.random.fold_in(rng, 6)
    for position, parts in split:
        steps = jnp.exp(jax.random.uniform(jax.random.fold_in(own, position), (parts,), jnp.float32, low / len(split), top_value / len(split)))
        factor_of = factor_of * jnp.repeat(steps, extent[position] // parts).reshape([-1 if axis == position else 1 for axis in range(len(extent))])
    return factor_of


def centred(own_key, dims, scale, limit, split=(), kind=jnp.bfloat16):
    gain = shard_levels(own_key, dims, split, -0.22, 0.18) if split else 1.0
    result = jax.random.normal(own_key, dims, jnp.float32) * scale * gain
    return jnp.minimum(jnp.maximum(result, -limit), limit).astype(kind)


def heavy_noise(stream_key, dims, width, reach, shards, heavy, kind=jnp.bfloat16):
    values = width * jax.random.normal(stream_key, dims, jnp.float32)
    if shards:
        values = values * shard_levels(stream_key, dims, shards, -0.22, 0.18)
    return jnp.clip(with_spikes(values, jax.random.fold_in(stream_key, 3), *heavy), -reach, reach).astype(kind)


def setup_inputs(seed: int = 0) -> dict:
    splits = jax.random.split(jax.random.key(seed), 25)
    slope_up = heavy_noise(splits[0], (REPLICAS, WIDTH, INNER), 0.5, 4.0, ((0, 16), (2, 2)), (0, 1, 16, 2.0), jnp.float32)
    slope_down = heavy_noise(splits[1], (REPLICAS, INNER, WIDTH), 0.5, 4.0, ((0, 16), (1, 2)), (0, 2, 16, 2.0), jnp.float32)
    slope_query = heavy_noise(splits[2], (REPLICAS, WIDTH, ATTN), 0.5, 4.0, ((0, 16), (2, 2)), (0, 1, 16, 2.0), jnp.float32)
    slope_key = heavy_noise(splits[3], (REPLICAS, WIDTH, ATTN), 0.5, 4.0, ((0, 16), (2, 2)), (0, 1, 16, 2.0), jnp.float32)
    slope_value = heavy_noise(splits[4], (REPLICAS, WIDTH, ATTN), 0.5, 4.0, ((0, 16), (2, 2)), (0, 1, 16, 2.0), jnp.float32)
    slope_mixed = heavy_noise(splits[5], (REPLICAS, ATTN, WIDTH), 0.5, 4.0, ((0, 16), (1, 2)), (0, 2, 16, 2.0), jnp.float32)
    slope_norm = heavy_noise(splits[6], (REPLICAS, WIDTH), 1.0, 8.0, ((0, 16),), (0, 1, 16, 2.0), jnp.float32)
    slope_bias = heavy_noise(splits[7], (REPLICAS, WIDTH), 1.0, 8.0, ((0, 16),), (0, 1, 16, 2.0), jnp.float32)
    param_up = heavy_noise(splits[8], (WIDTH, INNER), WIDTH ** -0.5, 0.3125, ((0, 16), (1, 2)), (1, 0, 16, 2.0), jnp.float32)
    param_down = heavy_noise(splits[9], (INNER, WIDTH), INNER ** -0.5, 0.15625, ((0, 2), (1, 16)), (0, 1, 16, 2.0), jnp.float32)
    param_query = heavy_noise(splits[10], (WIDTH, ATTN), WIDTH ** -0.5, 0.3125, ((0, 16), (1, 2)), (1, 0, 16, 2.0), jnp.float32)
    param_key = heavy_noise(splits[11], (WIDTH, ATTN), WIDTH ** -0.5, 0.3125, ((0, 16), (1, 2)), (1, 0, 16, 2.0), jnp.float32)
    param_value = heavy_noise(splits[12], (WIDTH, ATTN), WIDTH ** -0.5, 0.3125, ((0, 16), (1, 2)), (1, 0, 16, 2.0), jnp.float32)
    param_mixed = heavy_noise(splits[13], (ATTN, WIDTH), ATTN ** -0.5, 0.3125, ((0, 2), (1, 16)), (0, 1, 16, 2.0), jnp.float32)
    param_norm = jnp.clip(1.0 + 0.15 * jax.random.normal(splits[14], (WIDTH,), jnp.float32), 0.25, 1.75)
    param_bias = centred(splits[15], (WIDTH,), 0.5, 3.0, ((0, 16),), jnp.float32)
    state_up = jnp.clip(0.00026041668 + 0.00234375 * jax.random.uniform(splits[16], (WIDTH, INNER), jnp.float32) ** shard_levels(splits[16], (WIDTH, INNER), ((0, 16), (1, 2)), -0.2, 0.2), 0.00026041668, 0.0026041667)
    state_down = jnp.clip(6.510417006211355e-05 + 0.0005859375 * jax.random.uniform(splits[17], (INNER, WIDTH), jnp.float32) ** shard_levels(splits[17], (INNER, WIDTH), ((0, 2), (1, 16)), -0.2, 0.2), 6.510417006211355e-05, 0.0006510417)
    state_query = jnp.clip(0.00026041668 + 0.00234375 * jax.random.uniform(splits[18], (WIDTH, ATTN), jnp.float32) ** shard_levels(splits[18], (WIDTH, ATTN), ((0, 16), (1, 2)), -0.2, 0.2), 0.00026041668, 0.0026041667)
    state_key = jnp.clip(0.00026041668 + 0.00234375 * jax.random.uniform(splits[19], (WIDTH, ATTN), jnp.float32) ** shard_levels(splits[19], (WIDTH, ATTN), ((0, 16), (1, 2)), -0.2, 0.2), 0.00026041668, 0.0026041667)
    state_value = jnp.clip(0.00026041668 + 0.00234375 * jax.random.uniform(splits[20], (WIDTH, ATTN), jnp.float32) ** shard_levels(splits[20], (WIDTH, ATTN), ((0, 16), (1, 2)), -0.2, 0.2), 0.00026041668, 0.0026041667)
    state_mixed = jnp.clip(0.00026041668 + 0.00234375 * jax.random.uniform(splits[21], (ATTN, WIDTH), jnp.float32) ** shard_levels(splits[21], (ATTN, WIDTH), ((0, 2), (1, 16)), -0.2, 0.2), 0.00026041668, 0.0026041667)
    state_norm = jnp.clip(0.05 + 0.75 * jax.random.uniform(splits[22], (WIDTH,), jnp.float32) ** shard_levels(splits[22], (WIDTH,), ((0, 16),), -0.2, 0.2), 0.05, 0.8)
    state_bias = jnp.clip(0.05 + 0.75 * jax.random.uniform(splits[23], (WIDTH,), jnp.float32) ** shard_levels(splits[23], (WIDTH,), ((0, 16),), -0.2, 0.2), 0.05, 0.8)
    return dict(slope_up=slope_up, slope_down=slope_down, slope_query=slope_query, slope_key=slope_key, slope_value=slope_value, slope_mixed=slope_mixed, slope_norm=slope_norm, slope_bias=slope_bias, param_up=param_up, param_down=param_down, param_query=param_query, param_key=param_key, param_value=param_value, param_mixed=param_mixed, param_norm=param_norm, param_bias=param_bias, state_up=state_up, state_down=state_down, state_query=state_query, state_key=state_key, state_value=state_value, state_mixed=state_mixed, state_norm=state_norm, state_bias=state_bias)


learn_rate = 0.025
hold_rate = 0.7

def reference(slope_up, slope_down, slope_query, slope_key, slope_value, slope_mixed, slope_norm, slope_bias, param_up, param_down, param_query, param_key, param_value, param_mixed, param_norm, param_bias, state_up, state_down, state_query, state_key, state_value, state_mixed, state_norm, state_bias):
    mean_up = lax.optimization_barrier(jnp.sum(slope_up.astype(jnp.float32), axis=0)) * REPLICAS ** (-0.5)
    mean_down = lax.optimization_barrier(jnp.sum(slope_down.astype(jnp.float32), axis=0)) * REPLICAS ** (-0.5)
    mean_query = lax.optimization_barrier(jnp.sum(slope_query.astype(jnp.float32), axis=0)) * REPLICAS ** (-0.5)
    mean_key = lax.optimization_barrier(jnp.sum(slope_key.astype(jnp.float32), axis=0)) * REPLICAS ** (-0.5)
    mean_value = lax.optimization_barrier(jnp.sum(slope_value.astype(jnp.float32), axis=0)) * REPLICAS ** (-0.5)
    mean_mixed = lax.optimization_barrier(jnp.sum(slope_mixed.astype(jnp.float32), axis=0)) * REPLICAS ** (-0.5)
    mean_norm = lax.optimization_barrier(jnp.sum(slope_norm.astype(jnp.float32), axis=0)) * REPLICAS ** (-0.5)
    mean_bias = lax.optimization_barrier(jnp.sum(slope_bias.astype(jnp.float32), axis=0)) * REPLICAS ** (-0.5)
    ratio_up = jnp.sqrt(lax.optimization_barrier(jnp.sum(param_up * param_up, axis=1, keepdims=True))) * lax.rsqrt(lax.optimization_barrier(jnp.sum(mean_up * mean_up, axis=1, keepdims=True)) + 1e-06)
    mean_up = mean_up * ratio_up
    ratio_down = jnp.sqrt(lax.optimization_barrier(jnp.sum(param_down * param_down, axis=0, keepdims=True))) * lax.rsqrt(lax.optimization_barrier(jnp.sum(mean_down * mean_down, axis=0, keepdims=True)) + 1e-06)
    mean_down = mean_down * ratio_down
    ratio_query = jnp.sqrt(lax.optimization_barrier(jnp.sum(param_query * param_query, axis=1, keepdims=True))) * lax.rsqrt(lax.optimization_barrier(jnp.sum(mean_query * mean_query, axis=1, keepdims=True)) + 1e-06)
    mean_query = mean_query * ratio_query
    ratio_key = jnp.sqrt(lax.optimization_barrier(jnp.sum(param_key * param_key, axis=1, keepdims=True))) * lax.rsqrt(lax.optimization_barrier(jnp.sum(mean_key * mean_key, axis=1, keepdims=True)) + 1e-06)
    mean_key = mean_key * ratio_key
    ratio_value = jnp.sqrt(lax.optimization_barrier(jnp.sum(param_value * param_value, axis=1, keepdims=True))) * lax.rsqrt(lax.optimization_barrier(jnp.sum(mean_value * mean_value, axis=1, keepdims=True)) + 1e-06)
    mean_value = mean_value * ratio_value
    ratio_mixed = jnp.sqrt(lax.optimization_barrier(jnp.sum(param_mixed * param_mixed, axis=0, keepdims=True))) * lax.rsqrt(lax.optimization_barrier(jnp.sum(mean_mixed * mean_mixed, axis=0, keepdims=True)) + 1e-06)
    mean_mixed = mean_mixed * ratio_mixed
    state_new_up = hold_rate * state_up + (1.0 - hold_rate) * mean_up * mean_up
    next_up = param_up - learn_rate * mean_up * lax.rsqrt(state_new_up + 1e-06)
    state_new_down = hold_rate * state_down + (1.0 - hold_rate) * mean_down * mean_down
    next_down = param_down - learn_rate * mean_down * lax.rsqrt(state_new_down + 1e-06)
    state_new_query = hold_rate * state_query + (1.0 - hold_rate) * mean_query * mean_query
    next_query = param_query - learn_rate * mean_query * lax.rsqrt(state_new_query + 1e-06)
    state_new_key = hold_rate * state_key + (1.0 - hold_rate) * mean_key * mean_key
    next_key = param_key - learn_rate * mean_key * lax.rsqrt(state_new_key + 1e-06)
    state_new_value = hold_rate * state_value + (1.0 - hold_rate) * mean_value * mean_value
    next_value = param_value - learn_rate * mean_value * lax.rsqrt(state_new_value + 1e-06)
    state_new_mixed = hold_rate * state_mixed + (1.0 - hold_rate) * mean_mixed * mean_mixed
    next_mixed = param_mixed - learn_rate * mean_mixed * lax.rsqrt(state_new_mixed + 1e-06)
    state_new_norm = hold_rate * state_norm + (1.0 - hold_rate) * mean_norm * mean_norm
    next_norm = param_norm - learn_rate * mean_norm * lax.rsqrt(state_new_norm + 1e-06)
    state_new_bias = hold_rate * state_bias + (1.0 - hold_rate) * mean_bias * mean_bias
    next_bias = param_bias - learn_rate * mean_bias * lax.rsqrt(state_new_bias + 1e-06)
    half_up = next_up.astype(jnp.bfloat16)
    half_down = next_down.astype(jnp.bfloat16)
    half_query = next_query.astype(jnp.bfloat16)
    half_key = next_key.astype(jnp.bfloat16)
    half_value = next_value.astype(jnp.bfloat16)
    half_mixed = next_mixed.astype(jnp.bfloat16)
    half_norm = next_norm.astype(jnp.bfloat16)
    half_bias = next_bias.astype(jnp.bfloat16)
    return (half_up, half_down, half_query, half_key, half_value, half_mixed, half_norm, half_bias, next_up, next_down, next_query, next_key, next_value, next_mixed, next_norm, next_bias, state_new_up, state_new_down, state_new_query, state_new_key, state_new_value, state_new_mixed, state_new_norm, state_new_bias)
```

```python
import jax
import jax.numpy as jnp
from jax import lax
from jax.experimental import pallas as pl
from jax.sharding import PartitionSpec as P

learn_rate = 0.025
hold_rate = 0.7
LANES = 128
TURNED = (1, 5)


def lane_ceil(width):
    return -(-width // LANES) * LANES


def split_columns(packed, widths, steps):
    pieces, start = [], 0
    for width, step in zip(widths, steps):
        pieces.append(packed[:, start : start + width])
        start += step
    return pieces


def pack_kernel(*refs):
    out_ref = refs[-1]
    start = 0
    for at, ref in enumerate(refs[:-1]):
        block = ref[...].T if at in TURNED else ref[...]
        width = block.shape[1]
        out_ref[:, start : start + width] = block
        step = lane_ceil(width)
        if step > width:
            out_ref[:, start + width : start + step] = jnp.zeros(
                (block.shape[0], step - width), block.dtype
            )
        start += step


def pack_slopes(*arrays):
    rows = arrays[0].shape[1]
    tile = LANES if rows % LANES == 0 else rows
    specs, total = [], 0
    for at, array in enumerate(arrays):
        if at in TURNED:
            specs.append(pl.BlockSpec((None, array.shape[1], tile), lambda i: (0, 0, i)))
            total += lane_ceil(array.shape[1])
        elif array.ndim == 3:
            specs.append(pl.BlockSpec((None, tile, array.shape[2]), lambda i: (0, i, 0)))
            total += lane_ceil(array.shape[2])
        else:
            specs.append(pl.BlockSpec((tile, array.shape[1]), lambda i: (i, 0)))
            total += lane_ceil(array.shape[1])
    return pl.pallas_call(
        pack_kernel,
        grid=(rows // tile,),
        in_specs=specs,
        out_specs=pl.BlockSpec((tile, total), lambda i: (i, 0)),
        out_shape=jax.ShapeDtypeStruct((rows, total), jnp.float32),
        cost_estimate=pl.CostEstimate(
            flops=0, bytes_accessed=8 * rows * total, transcendentals=0
        ),
        name="pack_slopes",
    )(*arrays)


def scatter_sum(packed):
    return lax.psum_scatter(packed, "replica", scatter_dimension=0, tiled=True)


def gather_rows(packed):
    return lax.all_gather(packed, "replica", axis=0, tiled=True)


def on_device(
    slope_up,
    slope_down,
    slope_query,
    slope_key,
    slope_value,
    slope_mixed,
    slope_norm,
    slope_bias,
    param_up,
    param_down,
    param_query,
    param_key,
    param_value,
    param_mixed,
    param_norm,
    param_bias,
    state_up,
    state_down,
    state_query,
    state_key,
    state_value,
    state_mixed,
    state_norm,
    state_bias,
):
    packed = pack_slopes(
        slope_up,
        slope_down,
        slope_query,
        slope_key,
        slope_value,
        slope_mixed,
        jnp.pad(jnp.stack([slope_norm[0], slope_bias[0]], axis=1), ((0, 0), (0, LANES - 2))),
    )
    packed = scatter_sum(packed)
    widths = (
        slope_up.shape[2],
        slope_down.shape[1],
        slope_query.shape[2],
        slope_key.shape[2],
        slope_value.shape[2],
        slope_mixed.shape[1],
        1,
        1,
    )
    mean_up, mean_down, mean_query, mean_key, mean_value, mean_mixed, mean_norm, mean_bias = (
        split_columns(packed, widths, [lane_ceil(width) for width in widths[:6]] + [1, 1])
    )
    mean_down = mean_down.T
    mean_mixed = mean_mixed.T
    mean_norm = mean_norm[:, 0]
    mean_bias = mean_bias[:, 0]
    mean_rate = lax.axis_size("replica") ** (-0.5)
    mean_up = mean_up * mean_rate
    mean_down = mean_down * mean_rate
    mean_query = mean_query * mean_rate
    mean_key = mean_key * mean_rate
    mean_value = mean_value * mean_rate
    mean_mixed = mean_mixed * mean_rate
    mean_norm = mean_norm * mean_rate
    mean_bias = mean_bias * mean_rate
    (
        own_up,
        own_down,
        own_query,
        own_key,
        own_value,
        own_mixed,
        slope_up_norm,
        slope_down_norm,
        slope_query_norm,
        slope_key_norm,
        slope_value_norm,
        slope_mixed_norm,
    ) = lax.psum(
        (
            jnp.sum(param_up * param_up, axis=1, keepdims=True),
            jnp.sum(param_down * param_down, axis=0, keepdims=True),
            jnp.sum(param_query * param_query, axis=1, keepdims=True),
            jnp.sum(param_key * param_key, axis=1, keepdims=True),
            jnp.sum(param_value * param_value, axis=1, keepdims=True),
            jnp.sum(param_mixed * param_mixed, axis=0, keepdims=True),
            jnp.sum(mean_up * mean_up, axis=1, keepdims=True),
            jnp.sum(mean_down * mean_down, axis=0, keepdims=True),
            jnp.sum(mean_query * mean_query, axis=1, keepdims=True),
            jnp.sum(mean_key * mean_key, axis=1, keepdims=True),
            jnp.sum(mean_value * mean_value, axis=1, keepdims=True),
            jnp.sum(mean_mixed * mean_mixed, axis=0, keepdims=True),
        ),
        "model",
    )
    mean_up = mean_up * (jnp.sqrt(own_up) * lax.rsqrt(slope_up_norm + 1e-06))
    mean_down = mean_down * (jnp.sqrt(own_down) * lax.rsqrt(slope_down_norm + 1e-06))
    mean_query = mean_query * (jnp.sqrt(own_query) * lax.rsqrt(slope_query_norm + 1e-06))
    mean_key = mean_key * (jnp.sqrt(own_key) * lax.rsqrt(slope_key_norm + 1e-06))
    mean_value = mean_value * (jnp.sqrt(own_value) * lax.rsqrt(slope_value_norm + 1e-06))
    mean_mixed = mean_mixed * (jnp.sqrt(own_mixed) * lax.rsqrt(slope_mixed_norm + 1e-06))
    state_new_up = hold_rate * state_up + (1.0 - hold_rate) * mean_up * mean_up
    next_up = param_up - learn_rate * mean_up * lax.rsqrt(state_new_up + 1e-06)
    state_new_down = hold_rate * state_down + (1.0 - hold_rate) * mean_down * mean_down
    next_down = param_down - learn_rate * mean_down * lax.rsqrt(state_new_down + 1e-06)
    state_new_query = hold_rate * state_query + (1.0 - hold_rate) * mean_query * mean_query
    next_query = param_query - learn_rate * mean_query * lax.rsqrt(state_new_query + 1e-06)
    state_new_key = hold_rate * state_key + (1.0 - hold_rate) * mean_key * mean_key
    next_key = param_key - learn_rate * mean_key * lax.rsqrt(state_new_key + 1e-06)
    state_new_value = hold_rate * state_value + (1.0 - hold_rate) * mean_value * mean_value
    next_value = param_value - learn_rate * mean_value * lax.rsqrt(state_new_value + 1e-06)
    state_new_mixed = hold_rate * state_mixed + (1.0 - hold_rate) * mean_mixed * mean_mixed
    next_mixed = param_mixed - learn_rate * mean_mixed * lax.rsqrt(state_new_mixed + 1e-06)
    state_new_norm = hold_rate * state_norm + (1.0 - hold_rate) * mean_norm * mean_norm
    next_norm = param_norm - learn_rate * mean_norm * lax.rsqrt(state_new_norm + 1e-06)
    state_new_bias = hold_rate * state_bias + (1.0 - hold_rate) * mean_bias * mean_bias
    next_bias = param_bias - learn_rate * mean_bias * lax.rsqrt(state_new_bias + 1e-06)
    packed = jnp.concatenate(
        [
            next_up,
            next_down.T,
            next_query,
            next_key,
            next_value,
            next_mixed.T,
            next_norm[:, None],
            next_bias[:, None],
        ],
        axis=1,
    ).astype(jnp.bfloat16)
    packed = gather_rows(packed)
    half_up, half_down, half_query, half_key, half_value, half_mixed, half_norm, half_bias = (
        split_columns(packed, widths, widths)
    )
    half_down = half_down.T
    half_mixed = half_mixed.T
    half_norm = half_norm[:, 0]
    half_bias = half_bias[:, 0]
    return (
        half_up,
        half_down,
        half_query,
        half_key,
        half_value,
        half_mixed,
        half_norm,
        half_bias,
        next_up,
        next_down,
        next_query,
        next_key,
        next_value,
        next_mixed,
        next_norm,
        next_bias,
        state_new_up,
        state_new_down,
        state_new_query,
        state_new_key,
        state_new_value,
        state_new_mixed,
        state_new_norm,
        state_new_bias,
    )


def solution(mesh):
    return jax.shard_map(
        on_device,
        mesh=mesh,
        in_specs=(
            P("replica", None, "model"),
            P("replica", "model", None),
            P("replica", None, "model"),
            P("replica", None, "model"),
            P("replica", None, "model"),
            P("replica", "model", None),
            P("replica", None),
            P("replica", None),
            P("replica", "model"),
            P("model", "replica"),
            P("replica", "model"),
            P("replica", "model"),
            P("replica", "model"),
            P("model", "replica"),
            P("replica"),
            P("replica"),
            P("replica", "model"),
            P("model", "replica"),
            P("replica", "model"),
            P("replica", "model"),
            P("replica", "model"),
            P("model", "replica"),
            P("replica"),
            P("replica"),
        ),
        out_specs=(
            P(None, "model"),
            P("model", None),
            P(None, "model"),
            P(None, "model"),
            P(None, "model"),
            P("model", None),
            P(),
            P(),
            P("replica", "model"),
            P("model", "replica"),
            P("replica", "model"),
            P("replica", "model"),
            P("replica", "model"),
            P("model", "replica"),
            P("replica"),
            P("replica"),
            P("replica", "model"),
            P("model", "replica"),
            P("replica", "model"),
            P("replica", "model"),
            P("replica", "model"),
            P("model", "replica"),
            P("replica"),
            P("replica"),
        ),
        check_vma=False,
    )
```
